32 devices in a mesh: row: 8 (over z, y), col: 4 (over x, core).
Axes of the slice: x: 2, y: 2, z: 4, core: 2. Of those that a mesh axis runs over, the one named last changes fastest.
Arguments:
- hidden: bfloat16 [131072, 1024], P(('row', 'col')), may hold values from -6 to 6
- routes: int32 [64, 256], P(('row', 'col')), may hold values from 0 to 2047, as said below
- w_qkv: bfloat16 [1024, 3072], P('row', 'col'), may hold values from -0.1875 to 0.1875
- w_proj: bfloat16 [1024, 1024], P('row', 'col'), may hold values from -0.75 to 0.75
- w_up: bfloat16 [1024, 4096], P('row', 'col'), may hold values from -0.1875 to 0.1875
- w_down: bfloat16 [4096, 1024], P('row', 'col'), may hold values from -0.09375 to 0.09375
- attn_gain: bfloat16 [1024], P(('row', 'col')), may hold values from 0.5 to 1.5
- mlp_gain: bfloat16 [1024], P(('row', 'col')), may hold values from 0.5 to 1.5
- router: bfloat16 [1024], P(('row', 'col')), may hold values from -0.1875 to 0.1875
- cotangent: bfloat16 [131072, 1024], P(('row', 'col')), may hold values from -6 to 6
Outputs:
- layer_out: bfloat16 [131072, 1024], P(('row', 'col'))
- grad_hidden: float32 [131072, 1024], P(('row', 'col'))
- grad_qkv: float32 [1024, 3072], P('row', 'col')
- grad_proj: float32 [1024, 1024], P('row', 'col')
- grad_up: float32 [1024, 4096], P('row', 'col')
- grad_down: float32 [4096, 1024], P('row', 'col')
- grad_attngain: float32 [1024], P(('row', 'col'))
- grad_mlpgain: float32 [1024], P(('row', 'col'))
- grad_router: float32 [1024], P(('row', 'col'))
The draws below stay inside these ranges and needn't reach their ends.
Inputs may be any that keep to these rules, and one draw needn't show every extreme that they name: `routes`: each row lists 256 distinct positions of its sequence in increasing order.
All inputs are finite; a program needn't handle non-finite values.
Results may differ from the reference program's by a relative error of at most 0.019.
Values may be sent and summed in bfloat16 or wider, within the bound.
No kernel may reach another device: no remote copies, remote signals or barrier semaphores. Data moves between devices by JAX's collectives and lax.ppermute only.
A program may use at most 320 MiB of HBM per device.

```python
import jax
import jax.numpy as jnp
from jax import lax

D = 1024
HEADS = 16
HEAD_DIM = 64
FF = 4096
L = 2048
BLOCK = 256
CAP = 256
SEQS = 64
TOKENS = 131072


def draw_routes(key, part):
    seq_keys = jax.random.split(key, SEQS)

    def pick_one(one_key):
        shuffled = jax.random.permutation(one_key, L)
        return jnp.sort(shuffled[:CAP])
    return jax.vmap(pick_one)(seq_keys).astype(jnp.int32)


def with_spikes(array, rng, source, target, blocks, factor):
    def block_of(axis_at):
        return (jnp.arange(array.shape[axis_at]) // (array.shape[axis_at] // blocks)).reshape((-1,) + (1,) * (array.ndim - 1 - axis_at))

    near = jax.random.permutation(rng, blocks)[block_of(target)]
    other_side = (block_of(target) + blocks // 2) % blocks
    return jnp.where((block_of(source) == near) | (block_of(source) == other_side), factor * array, array)


def levels(own_key, shape, shards, least, high):
    loudness, own = 1.0, jax.random.fold_in(own_key, 6)
    for dim, shards_of in shards:
        draws = jnp.exp(jax.random.uniform(jax.random.fold_in(own, dim), (shards_of,), jnp.float32, least / len(shards), high / len(shards)))
        loudness = loudness * jnp.repeat(draws, shape[dim] // shards_of).reshape([-1 if axis == dim else 1 for axis in range(len(shape))])
    return loudness


def normal_values(key, dims, spread, limit, pieces=(), held_as=jnp.bfloat16):
    loudness = levels(key, dims, pieces, -0.22, 0.18) if pieces else 1.0
    drawn = jax.random.normal(key, dims, jnp.float32) * spread * loudness
    return jnp.minimum(jnp.maximum(drawn, -limit), limit).astype(held_as)


def bell_draw_with(key, dims, scale, reach, pieces, heavy, dtype=jnp.bfloat16):
    values = scale * jax.random.normal(key, dims, jnp.float32)
    if pieces:
        values = values * levels(key, dims, pieces, -0.22, 0.18)
    return jnp.clip(with_spikes(values, jax.random.fold_in(key, 3), *heavy), -reach, reach).astype(dtype)


def setup_inputs(seed: int = 0) -> dict:
    seeds = jax.random.split(jax.random.key(seed), 11)
    return {
        "hidden": normal_values(seeds[0], (TOKENS, D), 1.0, 6.0, ((0, 32),)),
        "routes": draw_routes(jax.random.fold_in(seeds[10], 71), 0),
        "w_qkv": normal_values(seeds[2], (D, 3 * D), D ** -0.5, 0.1875, ((0, 8), (1, 4))),
        "w_proj": normal_values(seeds[3], (D, D), (D // 16) ** -0.5, 0.75, ((0, 8), (1, 4))),
        "w_up": normal_values(seeds[4], (D, FF), D ** -0.5, 0.1875, ((0, 8), (1, 4))),
        "w_down": normal_values(seeds[5], (FF, D), FF ** -0.5, 0.09375, ((0, 8), (1, 4))),
        "attn_gain": jnp.clip(1.0 + 0.1 * jax.random.normal(seeds[6], (D,), jnp.float32), 0.5, 1.5).astype(jnp.bfloat16),
        "mlp_gain": jnp.clip(1.0 + 0.1 * jax.random.normal(seeds[7], (D,), jnp.float32), 0.5, 1.5).astype(jnp.bfloat16),
        "router": normal_values(seeds[8], (D,), D ** -0.5, 0.1875, ((0, 32),)),
        "cotangent": bell_draw_with(seeds[9], (TOKENS, D), 1.0, 6.0, ((0, 32),), (0, 1, 32, 2.75)),
    }


@jax.custom_vjp
def low(v):
    return lax.optimization_barrier(v.astype(jnp.bfloat16)).astype(jnp.float32)

@jax.custom_vjp
def low_back(v):
    return v

def low_keep(v):
    return (low(v), None)

def low_pass(kept, grad):
    return (grad,)

def back_keep(v):
    return (v, None)

def back_low(kept, grad):
    return (low(grad),)
low.defvjp(low_keep, low_pass)
low_back.defvjp(back_keep, back_low)
epsilon = 1e-05

def product(left, right):
    return jnp.dot(left, right, precision=lax.Precision.HIGHEST)

def rms_scale(value, gain_vec):
    return value * lax.rsqrt(lax.optimization_barrier(jnp.mean(value * value, axis=-1, keepdims=True)) + epsilon) * gain_vec

def layer(params, sequence, picked):
    qkv_mat, proj_mat, up_mat, down_mat, gain_attn, gain_mlp, router_vec = params
    routed = jnp.take(sequence, picked, axis=0)
    count = picked.shape[0]
    gating = jax.nn.sigmoid(jnp.dot(routed, router_vec, precision=lax.Precision.HIGHEST))
    normed = low(rms_scale(routed, gain_attn))
    projected = low(low_back(product(normed, qkv_mat)))
    split = projected.reshape(count, 3, HEADS, HEAD_DIM).transpose(1, 2, 0, 3)
    query, keys, values = (split[0], split[1], split[2])
    scores = jnp.einsum('hqd,hkd->hqk', query, keys, precision=lax.Precision.HIGHEST) * HEAD_DIM ** (-0.5)
    scores = low_back(scores)
    blocks = picked // BLOCK
    allowed = blocks[:, None] >= blocks[None, :]
    masked = jnp.where(allowed[None], scores, -1e+30)
    row_top = lax.optimization_barrier(jnp.max(masked, axis=-1, keepdims=True))
    expo = jnp.exp(masked - row_top)
    probs = expo / lax.optimization_barrier(jnp.sum(expo, axis=-1, keepdims=True))
    mixed = jnp.einsum('hqk,hkd->hqd', low(probs), values, precision=lax.Precision.HIGHEST)
    mixed = low(low_back(mixed.transpose(1, 0, 2).reshape(count, D)))
    attn_out = low_back(product(mixed, proj_mat))
    resid = routed + attn_out
    normed_two = low(rms_scale(resid, gain_mlp))
    pre_act = low_back(product(normed_two, up_mat))
    act_low = low(jax.nn.gelu(pre_act, approximate=False))
    mlp_out = low_back(product(act_low, down_mat))
    updated = routed + gating[:, None] * (attn_out + mlp_out)
    return sequence.at[picked].set(updated)

def reference(hidden, routes, w_qkv, w_proj, w_up, w_down, attn_gain, mlp_gain, router, cotangent):
    params = (w_qkv.astype(jnp.float32), w_proj.astype(jnp.float32), w_up.astype(jnp.float32), w_down.astype(jnp.float32), attn_gain.astype(jnp.float32), mlp_gain.astype(jnp.float32), router.astype(jnp.float32))

    def visit(carried, item):
        sequence, picked, seq_cot = item

        def forward(param_set, seq_value):
            return layer(param_set, seq_value, picked)
        result, pullback = jax.vjp(forward, params, sequence.astype(jnp.float32))
        grad_params, grad_seq = pullback(seq_cot.astype(jnp.float32))
        carried = jax.tree.map(lambda older, newer: older + newer, carried, grad_params)
        return (carried, (result.astype(jnp.bfloat16), grad_seq))
    zeros = tuple((jnp.zeros_like(param) for param in params))
    totals, (outputs, grads_seq) = lax.scan(visit, zeros, (hidden.reshape(SEQS, L, D), routes, cotangent.reshape(SEQS, L, D)))
    return (outputs.reshape(TOKENS, D), grads_seq.reshape(TOKENS, D), totals[0], totals[1], totals[2], totals[3], totals[4], totals[5], totals[6])
```

```python
import jax
import jax.numpy as jnp
from jax import lax
from jax.sharding import PartitionSpec as P

HEADS = 16
HEAD_DIM = 64
L = 2048
BLOCK = 256

epsilon = 1e-05
sqrt_half = 0.7071067811865476
inv_root_two_pi = 0.3989422804014327

BOTH = ("row", "col")
F32 = jnp.float32
BF16 = jnp.bfloat16


def phi_parts(z):
    cdf = 0.5 * (1.0 + lax.erf(z * sqrt_half))
    slope = cdf + z * jnp.exp(-0.5 * z * z) * inv_root_two_pi
    return cdf, slope


def gather_weight(shard):
    rows, cols = lax.axis_size("row"), lax.axis_size("col")
    blocks = lax.all_gather(shard, BOTH, axis=0, tiled=False)
    high, wide = shard.shape
    blocks = blocks.reshape(rows, cols, high, wide).transpose(0, 2, 1, 3)
    return blocks.reshape(rows * high, cols * wide)


def scatter_grad(grad):
    rows, cols = lax.axis_size("row"), lax.axis_size("col")
    high, wide = grad.shape[0] // rows, grad.shape[1] // cols
    blocks = grad.reshape(rows, high, cols, wide).transpose(0, 2, 1, 3)
    blocks = blocks.reshape(rows * cols * high, wide)
    mine = lax.psum_scatter(blocks, BOTH, scatter_dimension=0, tiled=True)
    return mine.astype(F32)


def dot(left, right):
    return jnp.dot(left, right, preferred_element_type=F32)


def dot_t(left, right):
    return lax.dot_general(left, right, (((1,), (1,)), ((), ())), preferred_element_type=F32)


def t_dot(left, right):
    return lax.dot_general(left, right, (((0,), (0,)), ((), ())), preferred_element_type=F32)


def on_device(hidden, routes, w_qkv, w_proj, w_up, w_down, attn_gain, mlp_gain, router, cotangent):
    n_dev = lax.axis_size("row") * lax.axis_size("col")
    width = hidden.shape[1]
    seqs = hidden.shape[0] // L
    cap = routes.shape[1]
    tokens = seqs * cap
    scale = HEAD_DIM ** (-0.5)

    small = jnp.stack([attn_gain, mlp_gain, router])
    small = lax.all_gather(small, BOTH, axis=1, tiled=True).astype(F32)
    gain_attn, gain_mlp, router_vec = small[0], small[1], small[2]
    qkv_mat = gather_weight(w_qkv)
    proj_mat = gather_weight(w_proj)
    up_mat = gather_weight(w_up)
    down_mat = gather_weight(w_down)

    picks = (routes[:, :, None] == lax.broadcasted_iota(jnp.int32, (1, 1, L), 2)).astype(BF16)
    hidden3 = hidden.reshape(seqs, L, width)
    cot3 = cotangent.reshape(seqs, L, width)
    is_routed = jnp.sum(picks, axis=1, dtype=F32) > 0.5
    x = jnp.einsum("scl,sld->scd", picks, hidden3, preferred_element_type=F32).reshape(tokens, width)
    g = jnp.einsum("scl,sld->scd", picks, cot3, preferred_element_type=F32).reshape(tokens, width)

    gate = jax.nn.sigmoid(jnp.sum(x * router_vec, axis=-1, keepdims=True))
    r1 = lax.rsqrt(jnp.mean(x * x, axis=-1, keepdims=True) + epsilon)
    n1 = x * r1
    a = (n1 * gain_attn).astype(BF16)
    qkv = dot(a, qkv_mat).astype(BF16)
    split = qkv.reshape(seqs, cap, 3, HEADS, HEAD_DIM).transpose(2, 0, 3, 1, 4)
    q, k, v = split[0], split[1], split[2]
    scores = jnp.einsum("shqd,shkd->shqk", q, k, preferred_element_type=F32) * scale
    blocks = routes // BLOCK
    allowed = blocks[:, :, None] >= blocks[:, None, :]
    masked = jnp.where(allowed[:, None], scores, -1e30)
    expo = jnp.exp(masked - jnp.max(masked, axis=-1, keepdims=True))
    probs = expo / jnp.sum(expo, axis=-1, keepdims=True)
    probs_low = probs.astype(BF16)
    mixed = jnp.einsum("shqk,shkd->shqd", probs_low, v, preferred_element_type=F32).astype(BF16)
    mixed = mixed.transpose(0, 2, 1, 3).reshape(tokens, width)
    attn = dot(mixed, proj_mat)
    u = x + attn
    r2 = lax.rsqrt(jnp.mean(u * u, axis=-1, keepdims=True) + epsilon)
    n2 = u * r2
    b = (n2 * gain_mlp).astype(BF16)
    z = dot(b, up_mat)
    cdf, slope = phi_parts(z)
    act = (z * cdf).astype(BF16)
    gmlp = (gate * g).astype(BF16)
    d_down = t_dot(act, gmlp).astype(BF16)
    out_down = scatter_grad(d_down)

    gz = (dot_t(gmlp, down_mat) * slope).astype(BF16)
    d_up = t_dot(b, gz).astype(BF16)
    out_up = scatter_grad(d_up)
    mlp = dot(act, down_mat)
    branch = attn + mlp
    gscore = jnp.sum(g * branch, axis=-1, keepdims=True) * gate * (1.0 - gate)

    gb = dot_t(gz, up_mat)
    t = gb * gain_mlp
    gu = r2 * (t - n2 * jnp.mean(t * n2, axis=-1, keepdims=True))
    gattn = (gate * g + gu).astype(BF16)
    d_proj = t_dot(mixed, gattn).astype(BF16)
    out_proj = scatter_grad(d_proj)
    gheads = dot_t(gattn, proj_mat).astype(BF16)
    gheads = gheads.reshape(seqs, cap, HEADS, HEAD_DIM).transpose(0, 2, 1, 3)
    gprobs = jnp.einsum("shqd,shkd->shqk", gheads, v, preferred_element_type=F32)
    gv = jnp.einsum("shqk,shqd->shkd", probs_low, gheads, preferred_element_type=F32)
    gs = (probs * (gprobs - jnp.sum(probs * gprobs, axis=-1, keepdims=True))).astype(BF16)
    gq = jnp.einsum("shqk,shkd->shqd", gs, k, preferred_element_type=F32) * scale
    gk = jnp.einsum("shqk,shqd->shkd", gs, q, preferred_element_type=F32) * scale
    gqkv = jnp.stack([gq, gk, gv]).astype(BF16).transpose(1, 3, 0, 2, 4).reshape(tokens, 3 * width)
    d_qkv = t_dot(a, gqkv).astype(BF16)
    out_qkv = scatter_grad(d_qkv)

    ga = dot_t(gqkv, qkv_mat)
    t1 = ga * gain_attn
    gx = g + gscore * router_vec + gu + r1 * (t1 - n1 * jnp.mean(t1 * n1, axis=-1, keepdims=True))
    small_grads = jnp.stack(
        [jnp.sum(ga * n1, axis=0), jnp.sum(gb * n2, axis=0), jnp.sum(gscore * x, axis=0)]
    )
    small_grads = small_grads.reshape(3, n_dev, width // n_dev).transpose(1, 0, 2)
    small_grads = lax.psum_scatter(
        small_grads.reshape(n_dev, 3 * (width // n_dev)), BOTH, scatter_dimension=0, tiled=True
    ).reshape(3, width // n_dev)

    updated = (x + gate * branch).astype(BF16).reshape(seqs, cap, width)
    placed = jnp.einsum("scl,scd->sld", picks, updated, preferred_element_type=F32).astype(BF16)
    layer_out = jnp.where(is_routed[:, :, None], placed, hidden3)
    gx_high = gx.astype(BF16)
    gx_low = (gx - gx_high.astype(F32)).astype(BF16)
    back = jnp.einsum(
        "scl,scd->sld", picks, gx_high.reshape(seqs, cap, width), preferred_element_type=F32
    ) + jnp.einsum("scl,scd->sld", picks, gx_low.reshape(seqs, cap, width), preferred_element_type=F32)
    grad_hidden = jnp.where(is_routed[:, :, None], back, cot3.astype(F32))
    return (
        layer_out.reshape(-1, width),
        grad_hidden.reshape(-1, width),
        out_qkv,
        out_proj,
        out_up,
        out_down,
        small_grads[0],
        small_grads[1],
        small_grads[2],
    )


def solution(mesh):
    rowcol = P(BOTH, None)
    weight = P("row", "col")
    vector = P(BOTH)
    return jax.shard_map(
        on_device,
        mesh=mesh,
        in_specs=(rowcol, rowcol, weight, weight, weight, weight, vector, vector, vector, rowcol),
        out_specs=(rowcol, rowcol, weight, weight, weight, weight, vector, vector, vector),
        check_vma=False,
    )
```
